32 devices in a mesh: dp: 8 (over z, core), seq: 4 (over y, x).
Axes of the slice: x: 2, y: 2, z: 4, core: 2. Of those that a mesh axis runs over, the one named last changes fastest.
Arguments:
- tokens: bfloat16 [32, 256, 1024], P(('dp', 'seq')), may hold values from -6 to 6
- queries: bfloat16 [32, 256, 1024], P(('dp', 'seq')), may hold values from -240 to 240
- keys: bfloat16 [32, 256, 1024], P(('dp', 'seq')), may hold values from -7 to 7
- values: bfloat16 [32, 256, 1024], P(('dp', 'seq')), may hold values from -6 to 6
- ln_gain: bfloat16 [1024], replicated, may hold values from 0.5 to 1.5
- mean_in: bfloat16 [1024, 2048], P(None, 'seq'), may hold values from -0.1875 to 0.1875
- sigma_in: bfloat16 [1024, 2048], P(None, 'seq'), may hold values from 0.0039978027 to 0.029907227
- noise_in: bfloat16 [1024, 2048], P(None, 'seq'), may hold values from -4 to 4
- mean_out: bfloat16 [2048, 1024], P('seq'), may hold values from -0.125 to 0.125
- sigma_out: bfloat16 [2048, 1024], P('seq'), may hold values from 0.0019989014 to 0.014953613
- noise_out: bfloat16 [2048, 1024], P('seq'), may hold values from -4 to 4
- flip_in: int32 [32, 1024], P('dp'), may hold values from -1 to 1, as said below
- flip_mid: int32 [32, 2048], P('dp', 'seq'), may hold values from -1 to 1, as said below
- flip_hidden: int32 [32, 2048], P('dp', 'seq'), may hold values from -1 to 1, as said below
- flip_out: int32 [32, 1024], P('dp'), may hold values from -1 to 1, as said below
- cotangent: bfloat16 [32, 256, 1024], P(('dp', 'seq')), may hold values from -0.75 to 0.75
Outputs:
- block_out: bfloat16 [32, 256, 1024], P(('dp', 'seq'))
- resid_grad: bfloat16 [32, 256, 1024], P(('dp', 'seq'))
- grad_mean_in: float32 [1024, 2048], P(None, 'seq')
- grad_sigma_in: float32 [1024, 2048], P(None, 'seq')
- grad_mean_out: float32 [2048, 1024], P('seq')
- grad_sigma_out: float32 [2048, 1024], P('seq')
The draws below stay inside these ranges and needn't reach their ends.
Inputs may be any that keep to these rules, and one draw needn't show every extreme that they name: `flip_in`: each entry is -1 or +1. `flip_mid`: each entry is -1 or +1. `flip_hidden`: each entry is -1 or +1. `flip_out`: each entry is -1 or +1.
All inputs are finite; a program needn't handle non-finite values.
Results may differ from the reference program's by a relative error of at most 0.018.
Values may be sent and summed in bfloat16 or wider, within the bound.
No kernel may reach another device: no remote copies, remote signals or barrier semaphores. Data moves between devices by JAX's collectives and lax.ppermute only.
A program may use at most 128 MiB of HBM per device.

```python
import math
import jax
import jax.numpy as jnp
from jax import lax

D = 1024
HEADS = 16
FF = 2048
PATCH = 256
IMAGES = 32
N_SEQ = 4


def query_key_pair(key):
    base = jax.random.fold_in(key, 4242)
    key_q, key_k = jax.random.split(base, 2)
    queries = jnp.clip(jax.random.normal(key_q, (IMAGES, PATCH, D), jnp.float32), -6.0, 6.0)
    keys = jnp.clip(jax.random.normal(key_k, (IMAGES, PATCH, D), jnp.float32), -6.0, 6.0)
    return (queries, keys)


def draw_queries(key, part):
    return query_key_pair(key)[0].astype(jnp.bfloat16)


def draw_keys(key, part):
    return query_key_pair(key)[1].astype(jnp.bfloat16)


def sign_table(key, salt, rows, cols):
    bits = jax.random.randint(jax.random.fold_in(key, salt), (rows, cols), 0, 2, jnp.int32)
    return 2 * bits - 1


def draw_flip_in(key, part):
    return sign_table(key, 11, IMAGES, D)


def draw_flip_mid(key, part):
    return sign_table(key, 23, IMAGES, FF)


def draw_flip_hidden(key, part):
    return sign_table(key, 37, IMAGES, FF)


def draw_flip_out(key, part):
    return sign_table(key, 53, IMAGES, D)


def levels(rng, extent, cuts, least, top_value):
    def one(dim, parts):
        heights = jax.random.uniform(jax.random.fold_in(jax.random.fold_in(rng, 6), dim), (parts,), jnp.float32, least / len(cuts), top_value / len(cuts))
        return jnp.repeat(jnp.exp(heights), extent[dim] // parts).reshape((-1,) + (1,) * (len(extent) - dim - 1))

    loudness = one(*cuts[0])
    for cut in cuts[1:]:
        loudness = loudness * one(*cut)
    return loudness


def gaussian(stream_key, extent, width, most, shards=(), kind=jnp.bfloat16):
    result = width * jax.random.normal(stream_key, extent, jnp.float32)
    if shards:
        result = result * levels(stream_key, extent, shards, -0.22, 0.18)
    return jnp.clip(result, -most, most).astype(kind)


def setup_inputs(seed: int = 0) -> dict:
    arg_keys = jax.random.split(jax.random.key(seed), 17)
    return {
        "tokens": gaussian(arg_keys[0], (IMAGES, PATCH, D), 1.0, 6.0, ((0, 32),)),
        "queries": draw_queries(jax.random.fold_in(arg_keys[16], 71), 0),
        "keys": draw_keys(jax.random.fold_in(arg_keys[16], 71), 0),
        "values": gaussian(arg_keys[3], (IMAGES, PATCH, D), 1.0, 6.0, ((0, 32),)),
        "ln_gain": jnp.clip(1.0 + 0.1 * jax.random.normal(arg_keys[4], (D,), jnp.float32), 0.5, 1.5).astype(jnp.bfloat16),
        "mean_in": gaussian(arg_keys[5], (D, FF), D ** -0.5, 0.1875, ((1, 4),)),
        "sigma_in": jnp.clip(jnp.exp(math.log(0.029907227) - 2.01235525 * jax.random.uniform(arg_keys[6], (D, FF), jnp.float32) ** levels(arg_keys[6], (D, FF), ((1, 4),), -0.2, 0.2)), 0.0039978027, 0.029907227).astype(jnp.bfloat16),
        "noise_in": gaussian(arg_keys[7], (D, FF), 1.0, 4.0, ((1, 4),)),
        "mean_out": gaussian(arg_keys[8], (FF, D), FF ** -0.5, 0.125, ((0, 4),)),
        "sigma_out": jnp.clip(jnp.exp(math.log(0.014953613) - 2.01235525 * jax.random.uniform(arg_keys[9], (FF, D), jnp.float32) ** levels(arg_keys[9], (FF, D), ((0, 4),), -0.2, 0.2)), 0.0019989014, 0.014953613).astype(jnp.bfloat16),
        "noise_out": gaussian(arg_keys[10], (FF, D), 1.0, 4.0, ((0, 4),)),
        "flip_in": draw_flip_in(jax.random.fold_in(arg_keys[16], 71), 0),
        "flip_mid": draw_flip_mid(jax.random.fold_in(arg_keys[16], 71), 0),
        "flip_hidden": draw_flip_hidden(jax.random.fold_in(arg_keys[16], 71), 0),
        "flip_out": draw_flip_out(jax.random.fold_in(arg_keys[16], 71), 0),
        "cotangent": gaussian(arg_keys[15], (IMAGES, PATCH, D), 0.125, 0.75, ((0, 32),)),
    }


def attend(query_img, key_img, value_img):
    head_dim = D // HEADS
    qf = query_img.astype(jnp.float32).reshape(PATCH, HEADS, head_dim)
    kf = key_img.astype(jnp.float32).reshape(PATCH, HEADS, head_dim)
    vf = value_img.astype(jnp.float32).reshape(PATCH, HEADS, head_dim)
    scores = jnp.einsum('qhe,khe->hqk', qf, kf) * head_dim ** (-0.5)
    top = lax.optimization_barrier(jnp.max(scores, axis=-1, keepdims=True))
    expd = jnp.exp(scores - top)
    total = lax.optimization_barrier(jnp.sum(expd, axis=-1))
    weights = expd.astype(jnp.bfloat16).astype(jnp.float32)
    outs = jnp.einsum('hqk,khe->qhe', weights, vf) / jnp.transpose(total)[:, :, None]
    return outs.reshape(PATCH, D).astype(jnp.bfloat16)

def gelu_slope(pre):
    cdf = 0.5 * (1.0 + lax.erf(pre * 0.7071067811865476))
    pdf = jnp.exp(-0.5 * pre * pre) * 0.3989422804014327
    return cdf + pre * pdf

def contract_first(left, right):
    return lax.dot_general(left, right, (((0,), (0,)), ((), ())), preferred_element_type=jnp.float32)

def contract_last(left, right):
    return lax.dot_general(left, right, (((1,), (1,)), ((), ())), preferred_element_type=jnp.float32)

def reference(tokens, queries, keys, values, ln_gain, mean_in, sigma_in, noise_in, mean_out, sigma_out, noise_out, flip_in, flip_mid, flip_hidden, flip_out, cotangent):
    bf = jnp.bfloat16
    f32 = jnp.float32
    attn_out = lax.map(lambda trio: attend(trio[0], trio[1], trio[2]), (queries, keys, values))
    resid = (tokens.astype(f32) + attn_out.astype(f32)).astype(bf)
    resid_f = resid.astype(f32)
    centered = resid_f - lax.optimization_barrier(jnp.mean(resid_f, axis=-1, keepdims=True))
    rstd = lax.rsqrt(lax.optimization_barrier(jnp.mean(centered * centered, axis=-1, keepdims=True)) + 1e-06)
    ahat = centered * rstd
    gain_f = ln_gain.astype(f32)
    normed = (ahat * gain_f).astype(bf)
    pert_in = (sigma_in.astype(f32) * noise_in.astype(f32)).astype(bf)
    pert_out = (sigma_out.astype(f32) * noise_out.astype(f32)).astype(bf)
    in_signs = flip_in.astype(bf)[:, None, :]
    mid_signs = flip_mid.astype(f32)[:, None, :]
    hid_signs = flip_hidden.astype(bf)[:, None, :]
    out_signs = flip_out.astype(f32)[:, None, :]
    rows = PATCH * IMAGES
    flat = normed.reshape(rows, D)
    flat_flip = (normed * in_signs).reshape(rows, D)
    pre = jnp.dot(flat, mean_in, preferred_element_type=f32).reshape(IMAGES, PATCH, FF)
    pre = pre + jnp.dot(flat_flip, pert_in, preferred_element_type=f32).reshape(IMAGES, PATCH, FF) * mid_signs
    hidden = jax.nn.gelu(pre, approximate=False).astype(bf)
    flipped_hidden = hidden * hid_signs
    block = FF // N_SEQ
    mixed = jnp.zeros((IMAGES, PATCH, D), f32)
    for index in range(N_SEQ):
        lo = index * block
        hb = hidden[:, :, lo:lo + block].reshape(rows, block)
        hfb = flipped_hidden[:, :, lo:lo + block].reshape(rows, block)
        part = jnp.dot(hb, mean_out[lo:lo + block], preferred_element_type=f32).reshape(IMAGES, PATCH, D)
        part = part + jnp.dot(hfb, pert_out[lo:lo + block], preferred_element_type=f32).reshape(IMAGES, PATCH, D) * out_signs
        mixed = mixed + part.astype(bf).astype(f32)
    block_out = (resid_f + mixed).astype(bf)
    cot_flip = cotangent * flip_out.astype(bf)[:, None, :]
    cot_flat = cotangent.reshape(rows, D)
    cot_flip_flat = cot_flip.reshape(rows, D)
    dhidden = contract_last(cot_flat, mean_out).reshape(IMAGES, PATCH, FF)
    dhidden = dhidden + contract_last(cot_flip_flat, pert_out).reshape(IMAGES, PATCH, FF) * flip_hidden.astype(f32)[:, None, :]
    dpre = (dhidden * gelu_slope(pre)).astype(bf)
    dpre_flip = dpre * flip_mid.astype(bf)[:, None, :]
    grad_mean_out = contract_first(hidden.reshape(rows, FF), cot_flat)
    grad_sigma_out = contract_first(flipped_hidden.reshape(rows, FF), cot_flip_flat) * noise_out.astype(f32)
    grad_mean_in = contract_first(flat, dpre.reshape(rows, FF))
    grad_sigma_in = contract_first(flat_flip, dpre_flip.reshape(rows, FF)) * noise_in.astype(f32)
    dnormed = jnp.zeros((IMAGES, PATCH, D), f32)
    in_signs_f = flip_in.astype(f32)[:, None, :]
    for index in range(N_SEQ):
        lo = index * block
        db = dpre[:, :, lo:lo + block].reshape(rows, block)
        dfb = dpre_flip[:, :, lo:lo + block].reshape(rows, block)
        part = contract_last(db, mean_in[:, lo:lo + block]).reshape(IMAGES, PATCH, D)
        part = part + contract_last(dfb, pert_in[:, lo:lo + block]).reshape(IMAGES, PATCH, D) * in_signs_f
        dnormed = dnormed + part.astype(bf).astype(f32)
    scaled = dnormed * gain_f
    back = rstd * (scaled - lax.optimization_barrier(jnp.mean(scaled, axis=-1, keepdims=True)) - ahat * lax.optimization_barrier(jnp.mean(scaled * ahat, axis=-1, keepdims=True)))
    resid_grad = (cotangent.astype(f32) + back).astype(bf)
    return (block_out, resid_grad, grad_mean_in, grad_sigma_in, grad_mean_out, grad_sigma_out)
```

```python
import functools

import jax
import jax.numpy as jnp
from jax import lax
from jax.experimental import pallas as pl
from jax.experimental.pallas import tpu as pltpu
from jax.sharding import PartitionSpec as P

HEADS = 16
BF = jnp.bfloat16
F32 = jnp.float32
VMEM = pl.BlockSpec(memory_space=pltpu.VMEM)

NT = (((1,), (1,)), ((), ()))
NN = (((1,), (0,)), ((), ()))
TN = (((0,), (0,)), ((), ()))


def dot(a, b, dims):
    return lax.dot_general(a, b, dims, preferred_element_type=F32)


def relative(index, step, count):
    return index ^ step if count & (count - 1) == 0 else (index + step) % count


def pairs(step, count):
    return [(relative(i, step, count), i) for i in range(count)]


def back_pairs(step, count):
    return [(i, relative(i, step, count)) for i in range(count)]


def sign_rows(ref, step, own, seq):
    row = relative(lax.axis_index("seq"), step, seq) * own
    return ref[pl.ds(row, own), :]


def by_image(x, sign, own):
    rows, width = x.shape
    return (x.reshape(own, rows // own, width) * sign[:, None, :]).reshape(rows, width)


def mlp_kernel(step, own, seq, n_ref, c_ref, mi, pi, mo, po, fi, fm, fh, fo, h_ref, d_ref):
    n = n_ref[...]
    c = c_ref[...]
    si = sign_rows(fi, step, own, seq).astype(BF)
    sm = sign_rows(fm, step, own, seq).astype(F32)
    sh = sign_rows(fh, step, own, seq).astype(F32)
    so = sign_rows(fo, step, own, seq).astype(BF)
    pre = dot(n, mi[...], NN) + by_image(dot(by_image(n, si, own), pi[...], NN), sm, own)
    dh = dot(c, mo[...], NT) + by_image(dot(by_image(c, so, own), po[...], NT), sh, own)
    cdf = 0.5 * (1.0 + lax.erf(pre * 0.7071067811865476))
    pdf = jnp.exp(-0.5 * pre * pre) * 0.3989422804014327
    h_ref[...] = (pre * cdf).astype(BF)
    d_ref[...] = (dh * (cdf + pre * pdf)).astype(BF)


def partial_kernel(step, own, seq, h_ref, d_ref, mi, pi, mo, po, fi, fm, fh, fo, m_ref, g_ref):
    h = h_ref[...]
    d = d_ref[...]
    si = sign_rows(fi, step, own, seq).astype(F32)
    sm = sign_rows(fm, step, own, seq).astype(BF)
    sh = sign_rows(fh, step, own, seq).astype(BF)
    so = sign_rows(fo, step, own, seq).astype(F32)
    m_ref[...] = (dot(h, mo[...], NN) + by_image(dot(by_image(h, sh, own), po[...], NN), so, own)).astype(BF)
    g_ref[...] = (dot(d, mi[...], NT) + by_image(dot(by_image(d, sm, own), pi[...], NT), si, own)).astype(BF)


def grad_kernel(own, seq, left_sign, right_sign, noise, *refs):
    lefts = refs[:seq]
    rights = refs[seq : 2 * seq]
    mean_ref, sigma_ref = refs[2 * seq :]
    mean = None
    sigma = None
    for step in range(seq):
        a = lefts[step][...]
        b = rights[step][...]
        fa = by_image(a, sign_rows(left_sign, step, own, seq).astype(BF), own)
        fb = by_image(b, sign_rows(right_sign, step, own, seq).astype(BF), own)
        m = dot(a, b, TN)
        s = dot(fa, fb, TN)
        mean = m if mean is None else mean + m
        sigma = s if sigma is None else sigma + s
    mean_ref[...] = mean.astype(BF)
    sigma_ref[...] = (sigma * noise[...].astype(F32)).astype(BF)


def call(kernel, outs, args, flops):
    return pl.pallas_call(
        kernel,
        in_specs=[VMEM] * len(args),
        out_specs=[VMEM] * len(outs),
        out_shape=outs,
        compiler_params=pltpu.CompilerParams(vmem_limit_bytes=40 * 1024 * 1024),
        cost_estimate=pl.CostEstimate(flops=flops, transcendentals=0, bytes_accessed=0),
    )(*args)


def gather(v, seq):
    if seq != 4:
        return [v] + [lax.ppermute(v, "seq", pairs(r, seq)) for r in range(1, seq)]
    half = v.shape[0] // 2
    one = lax.ppermute(v, "seq", pairs(1, seq))
    two = lax.ppermute(v, "seq", pairs(2, seq))
    low = lax.ppermute(one[:half], "seq", pairs(2, seq))
    high = lax.ppermute(two[half:], "seq", pairs(1, seq))
    return [v, one, two, jnp.concatenate([low, high], axis=0)]


def scatter_sum(parts, seq):
    out = parts[0].astype(F32)
    for r in range(1, seq):
        out = out + lax.ppermute(parts[r], "seq", back_pairs(r, seq)).astype(F32)
    return out


def line_sum(v, cores, n):
    def shift(pairs_of_places, x):
        perm = [(a * cores + c, b * cores + c) for a, b in pairs_of_places for c in range(cores)]
        return lax.ppermute(x, "dp", perm)

    place = lax.axis_index("dp") // cores
    if n % 2:
        total = v.astype(F32)
        for k in range(1, n):
            total = total + shift([(a, (a + k) % n) for a in range(n)], v).astype(F32)
        return total.astype(BF)
    half = n // 2
    acc = v
    for k in range(half - 1):
        got = shift([(k, k + 1), (n - 1 - k, n - 2 - k)], acc)
        acc = (acc.astype(F32) + got.astype(F32)).astype(BF)
    got = shift([(half - 1, half), (half, half - 1)], acc)
    acc = (acc.astype(F32) + got.astype(F32)).astype(BF)
    for k in range(half - 2, -1, -1):
        got = shift([(k + 1, k), (n - 2 - k, n - 1 - k)], acc)
        acc = jnp.where((place == k) | (place == n - 1 - k), got, acc)
    return acc


def grad_sum(v, dp):
    cores = 2
    if dp % cores:
        return line_sum(v, 1, dp).astype(F32)
    core = lax.axis_index("dp") % cores
    swap = [(d, d ^ 1) for d in range(dp)]
    half = v.shape[0] // 2
    mine = jnp.where(core == 0, v[:half], v[half:])
    other = jnp.where(core == 0, v[half:], v[:half])
    got = lax.ppermute(other, "dp", swap)
    acc = (mine.astype(F32) + got.astype(F32)).astype(BF)
    acc = line_sum(acc, cores, dp // cores)
    got = lax.ppermute(acc, "dp", swap)
    low = jnp.where(core == 0, acc, got)
    high = jnp.where(core == 0, got, acc)
    return jnp.concatenate([low, high], axis=0).astype(F32)


def body(
    tokens,
    queries,
    keys,
    values,
    ln_gain,
    mean_in,
    sigma_in,
    noise_in,
    mean_out,
    sigma_out,
    noise_out,
    flip_in,
    flip_mid,
    flip_hidden,
    flip_out,
    cotangent,
):
    own, patches, width = tokens.shape
    rows = own * patches
    seq = lax.axis_size("seq")
    dp = lax.axis_size("dp")
    hidden_local = mean_in.shape[1]
    head_dim = width // HEADS
    scale = head_dim ** (-0.5)

    cot = gather(cotangent.reshape(rows, width), seq)

    pert_in = (sigma_in.astype(F32) * noise_in.astype(F32)).astype(BF)
    pert_out = (sigma_out.astype(F32) * noise_out.astype(F32)).astype(BF)
    query_heads = queries.reshape(own, patches, HEADS, head_dim)
    key_heads = keys.reshape(own, patches, HEADS, head_dim)
    value_heads = values.reshape(own, patches, HEADS, head_dim)
    scores = jnp.einsum("bqhe,bkhe->bhqk", query_heads, key_heads, preferred_element_type=F32) * scale
    top = jnp.max(scores, axis=-1, keepdims=True)
    expd = jnp.exp(scores - top)
    total = jnp.sum(expd, axis=-1)
    accum = jnp.einsum("bhqk,bkhe->bqhe", expd.astype(BF), value_heads, preferred_element_type=F32)
    attn_out = (accum / jnp.transpose(total, (0, 2, 1))[..., None]).reshape(own, patches, width).astype(BF)
    resid = (tokens.astype(F32) + attn_out.astype(F32)).astype(BF)
    resid_f = resid.astype(F32)
    centered = resid_f - jnp.mean(resid_f, axis=-1, keepdims=True)
    rstd = lax.rsqrt(jnp.mean(centered * centered, axis=-1, keepdims=True) + 1e-06)
    ahat = centered * rstd
    gain_f = ln_gain.astype(F32)
    normed = (ahat * gain_f).astype(BF)

    act = gather(normed.reshape(rows, width), seq)

    weights = (mean_in, pert_in, mean_out, pert_out)
    flips = (flip_in, flip_mid, flip_hidden, flip_out)
    flop = 8 * rows * width * hidden_local
    small = jax.ShapeDtypeStruct((rows, hidden_local), BF)
    big = jax.ShapeDtypeStruct((rows, width), BF)
    hidden, dpre = [], []
    for r in range(seq):
        h, d = call(functools.partial(mlp_kernel, r, own, seq), [small, small], (act[r], cot[r], *weights, *flips), flop)
        hidden.append(h)
        dpre.append(d)

    grad = functools.partial(grad_kernel, own, seq)
    out_w = jax.ShapeDtypeStruct((hidden_local, width), BF)
    in_w = jax.ShapeDtypeStruct((width, hidden_local), BF)
    g_mean_out, g_sigma_out = call(grad, [out_w, out_w], (flip_hidden, flip_out, noise_out, *hidden, *cot), seq * flop // 2)
    g_mean_in, g_sigma_in = call(grad, [in_w, in_w], (flip_in, flip_mid, noise_in, *act, *dpre), seq * flop // 2)

    mixed_parts, dn_parts = [], []
    for r in range(seq):
        m, g = call(functools.partial(partial_kernel, r, own, seq), [big, big], (hidden[r], dpre[r], *weights, *flips), flop)
        mixed_parts.append(m)
        dn_parts.append(g)

    grads = [grad_sum(g, dp) for g in (g_mean_out, g_sigma_out, g_mean_in, g_sigma_in)]
    mixed = scatter_sum(mixed_parts, seq).reshape(own, patches, width)
    dnormed = scatter_sum(dn_parts, seq).reshape(own, patches, width)
    block_out = (resid_f + mixed).astype(BF)
    scaled = dnormed * gain_f
    back = rstd * (
        scaled
        - jnp.mean(scaled, axis=-1, keepdims=True)
        - ahat * jnp.mean(scaled * ahat, axis=-1, keepdims=True)
    )
    resid_grad = (cotangent.astype(F32) + back).astype(BF)
    return (block_out, resid_grad, grads[2], grads[3], grads[0], grads[1])


def solution(mesh):
    img = P(("dp", "seq"), None, None)
    return jax.shard_map(
        body,
        mesh=mesh,
        in_specs=(
            img,
            img,
            img,
            img,
            P(),
            P(None, "seq"),
            P(None, "seq"),
            P(None, "seq"),
            P("seq", None),
            P("seq", None),
            P("seq", None),
            P("dp", None),
            P("dp", "seq"),
            P("dp", "seq"),
            P("dp", None),
            img,
        ),
        out_specs=(img, img, P(None, "seq"), P(None, "seq"), P("seq", None), P("seq", None)),
        check_vma=False,
    )
```

```python
import functools

import jax
import jax.numpy as jnp
from jax import lax
from jax.experimental import pallas as pl
from jax.experimental.pallas import tpu as pltpu
from jax.sharding import PartitionSpec as P


HEADS = 16
CORES = 2
LANES = 128
BF = jnp.bfloat16
F32 = jnp.float32
VMEM = pl.BlockSpec(memory_space=pltpu.VMEM)
LIMIT = 16 * 1024 * 1024
PIECES = 2

NT = (((1,), (1,)), ((), ()))
NN = (((1,), (0,)), ((), ()))
TN = (((0,), (0,)), ((), ()))


def dot(a, b, dims):
    return lax.dot_general(a, b, dims, preferred_element_type=F32)


def relative(index, step, count):
    return index ^ step if count & (count - 1) == 0 else (index + step) % count


def fetch(v, step, seq):
    return lax.ppermute(v, "seq", [(relative(i, step, seq), i) for i in range(seq)])


def give(v, step, seq):
    return lax.ppermute(v, "seq", [(i, relative(i, step, seq)) for i in range(seq)])


def sign_rows(ref, step, own, seq):
    row = relative(lax.axis_index("seq"), step, seq) * own
    return ref[pl.ds(row, own), :]


def by_image(x, sign, own):
    rows, width = x.shape
    return (x.reshape(own, rows // own, width) * sign[:, None, :]).reshape(rows, width)


def attention_kernel(own, t_ref, q_ref, k_ref, v_ref, g_ref, r_ref, n_ref):
    rows, width = t_ref.shape
    patches = rows // own
    head_dim = width // HEADS
    block = max(LANES, head_dim)
    scale = head_dim ** (-0.5)
    lane = lax.broadcasted_iota(jnp.int32, (patches, block), 1) // head_dim
    for b in range(own):
        at = slice(b * patches, (b + 1) * patches)
        for lo in range(0, width, block):
            q = q_ref[at, lo : lo + block]
            k = k_ref[at, lo : lo + block]
            v = v_ref[at, lo : lo + block]
            out = None
            for j in range(block // head_dim):
                kj = jnp.where(lane == j, k, jnp.zeros_like(k))
                vj = jnp.where(lane == j, v, jnp.zeros_like(v))
                s = dot(q, kj, NT) * scale
                e = jnp.exp(s - jnp.max(s, axis=-1, keepdims=True))
                o = dot(e.astype(BF), vj, NN) / jnp.sum(e, axis=-1, keepdims=True)
                out = o if out is None else out + o
            attn = out.astype(BF).astype(F32)
            r_ref[at, lo : lo + block] = (t_ref[at, lo : lo + block].astype(F32) + attn).astype(BF)
    x = r_ref[...].astype(F32)
    c = x - jnp.mean(x, axis=-1, keepdims=True)
    rstd = lax.rsqrt(jnp.mean(c * c, axis=-1, keepdims=True) + 1e-06)
    n_ref[...] = (c * rstd * g_ref[...].astype(F32)[None, :]).astype(BF)


def perturb_kernel(si, ni, so, no, pi, po):
    pi[...] = (si[...].astype(F32) * ni[...].astype(F32)).astype(BF)
    po[...] = (so[...].astype(F32) * no[...].astype(F32)).astype(BF)


def mlp_kernel(step, own, seq, n_ref, c_ref, mi, pi, mo, po, fi, fm, fh, fo, h_ref, d_ref):
    n = n_ref[...]
    c = c_ref[...]
    si = sign_rows(fi, step, own, seq).astype(BF)
    sm = sign_rows(fm, step, own, seq).astype(F32)
    sh = sign_rows(fh, step, own, seq).astype(F32)
    so = sign_rows(fo, step, own, seq).astype(BF)
    pre = dot(n, mi[...], NN) + by_image(dot(by_image(n, si, own), pi[...], NN), sm, own)
    dh = dot(c, mo[...], NT) + by_image(dot(by_image(c, so, own), po[...], NT), sh, own)
    cdf = 0.5 * (1.0 + lax.erf(pre * 0.7071067811865476))
    pdf = jnp.exp(-0.5 * pre * pre) * 0.3989422804014327
    h_ref[...] = (pre * cdf).astype(BF)
    d_ref[...] = (dh * (cdf + pre * pdf)).astype(BF)


def partial_kernel(step, own, seq, h_ref, d_ref, mi, pi, mo, po, fi, fm, fh, fo, out):
    h = h_ref[...]
    d = d_ref[...]
    si = sign_rows(fi, step, own, seq).astype(F32)
    sm = sign_rows(fm, step, own, seq).astype(BF)
    sh = sign_rows(fh, step, own, seq).astype(BF)
    so = sign_rows(fo, step, own, seq).astype(F32)
    rows = h.shape[0]
    out[:rows] = (dot(h, mo[...], NN) + by_image(dot(by_image(h, sh, own), po[...], NN), so, own)).astype(BF)
    out[rows:] = (dot(d, mi[...], NT) + by_image(dot(by_image(d, sm, own), pi[...], NT), si, own)).astype(BF)


def products(steps, own, seq, left_sign, right_sign, lefts, rights):
    mean = sigma = None
    for step, left, right in zip(steps, lefts, rights):
        a = left[...]
        b = right[...]
        fa = by_image(a, sign_rows(left_sign, step, own, seq).astype(BF), own)
        fb = by_image(b, sign_rows(right_sign, step, own, seq).astype(BF), own)
        m = dot(a, b, TN)
        s = dot(fa, fb, TN)
        mean = m if mean is None else mean + m
        sigma = s if sigma is None else sigma + s
    return mean, sigma


def early_kernel(steps, own, seq, left_sign, right_sign, *refs):
    n = len(steps)
    mean, sigma = products(steps, own, seq, left_sign, right_sign, refs[:n], refs[n : 2 * n])
    refs[-2][...] = mean
    refs[-1][...] = sigma


def late_kernel(step, own, seq, axis, flipped, left_sign, right_sign, noise, so_far, left, right, keep, send):
    a = left[...]
    b = right[...]
    if flipped:
        a = by_image(a, sign_rows(left_sign, step, own, seq).astype(BF), own)
        b = by_image(b, sign_rows(right_sign, step, own, seq).astype(BF), own)
    full = so_far[...] + dot(a, b, TN)
    if flipped:
        full = full * noise[...].astype(F32)
    full = full.astype(BF)
    half = full.shape[axis] // 2
    low, high = (full[:half], full[half:]) if axis == 0 else (full[:, :half], full[:, half:])
    first = lax.axis_index("dp") % CORES == 0
    keep[...] = jnp.where(first, low, high)
    send[...] = jnp.where(first, high, low)


def assemble_kernel(mine, other, *refs):
    out = refs[-1]
    here = lax.axis_index("dp") % CORES == pl.program_id(0)
    out[...] = jnp.where(here, mine[...], other[...]).astype(F32)


def plus(a, b):
    return (a.astype(F32) + b.astype(F32)).astype(BF)


def at_end():
    place = lax.axis_index("dp") // CORES
    return (place == 0) | (place == lax.axis_size("dp") // CORES - 1)


def split_kernel(keep, got, *outs):
    rows = outs[0].shape[0]
    for i, out in enumerate(outs):
        at = slice(i * rows, (i + 1) * rows)
        out[...] = plus(keep[at, :], got[at, :])


def edge_kernel(got, piece, done, half, out):
    half[...] = plus(piece[...], got[...])
    out[...] = jnp.where(at_end(), got[...], done[...])


def plus_kernel(a, b, out):
    out[...] = plus(a[...], b[...])


def choose_kernel(a, b, out):
    out[...] = jnp.where(at_end(), a[...], b[...])


def middle_kernel(half, got, piece, done, x):
    total = plus(half[...], got[...])
    done[...] = total
    x[...] = jnp.where(at_end(), piece[...], total)


def norm_back_kernel(seq, r_ref, c_ref, g_ref, *refs):
    rows = r_ref.shape[0]
    both = refs[0][...].astype(F32)
    for i in range(1, seq):
        both = both + refs[i][...].astype(F32)
    mixed = both[:rows]
    dn = both[rows:]
    x = r_ref[...].astype(F32)
    refs[-2][...] = (x + mixed).astype(BF)
    c = x - jnp.mean(x, axis=-1, keepdims=True)
    rstd = lax.rsqrt(jnp.mean(c * c, axis=-1, keepdims=True) + 1e-06)
    ahat = c * rstd
    g = dn * g_ref[...].astype(F32)[None, :]
    back = rstd * (g - jnp.mean(g, axis=-1, keepdims=True) - ahat * jnp.mean(g * ahat, axis=-1, keepdims=True))
    refs[-1][...] = (c_ref[...].astype(F32) + back).astype(BF)


def block_of(axis, piece, half):
    return (half * PIECES + piece, 0) if axis == 0 else (piece, half)


def call(kernel, outs, args, flops, **more):
    more.setdefault("in_specs", [VMEM] * len(args))
    more.setdefault("out_specs", [VMEM] * len(outs))
    return pl.pallas_call(
        kernel,
        out_shape=outs,
        compiler_params=pltpu.CompilerParams(vmem_limit_bytes=LIMIT),
        cost_estimate=pl.CostEstimate(flops=flops, transcendentals=0, bytes_accessed=0),
        **more,
    )(*args)


def gather(v, seq, relayed):
    if seq != 4:
        return [v] + [fetch(v, r, seq) for r in range(1, seq)]
    one = fetch(v, 1, seq)
    two = fetch(v, 2, seq)
    last = fetch(one if relayed == 1 else two, 3 - relayed, seq)
    return [v, one, two, last]


def places(moves, swapped=()):
    perm = [(a * CORES + c, b * CORES + c) for a, b in moves for c in range(CORES)]
    return perm + [(a * CORES + c, a * CORES + CORES - 1 - c) for a in swapped for c in range(CORES)]


def along(moves, x, swapped=()):
    return lax.ppermute(x, "dp", places(moves, swapped))


def line_sum(v, n):
    place = lax.axis_index("dp") // CORES
    if n % 2:
        total = v.astype(F32)
        for k in range(1, n):
            total = total + along([(a, (a + k) % n) for a in range(n)], v).astype(F32)
        return total.astype(BF)
    half = n // 2
    acc = v
    for k in range(half - 1):
        acc = plus(acc, along([(k, k + 1), (n - 1 - k, n - 2 - k)], acc))
    acc = plus(acc, along([(half - 1, half), (half, half - 1)], acc))
    for k in range(half - 2, -1, -1):
        got = along([(k + 1, k), (n - 2 - k, n - 1 - k)], acc)
        acc = jnp.where((place == k) | (place == n - 1 - k), got, acc)
    return acc


def four_line_sums(pieces, lag=3):
    count = len(pieces)
    like = jax.ShapeDtypeStruct(pieces[0].shape, BF)
    halves, sums, ready, out = [None] * count, [None] * count, list(pieces), [None] * count
    for k in range(count + lag):
        got = along([(0, 1), (1, 0), (2, 3), (3, 2)], ready[k])
        if lag <= k < count:
            halves[k], out[k - lag] = call(edge_kernel, [like, like], (got, pieces[k], sums[k - lag]), like.size)
        elif k < lag:
            halves[k] = call(plus_kernel, [like], (pieces[k], got), like.size)[0]
        else:
            out[k - lag] = call(choose_kernel, [like], (got, sums[k - lag]), like.size)[0]
        if k < count:
            other = along([(1, 2), (2, 1)], halves[k], (0, 3))
            if k + lag < count:
                sums[k], ready[k + lag] = call(middle_kernel, [like, like], (halves[k], other, pieces[k + lag]), like.size)
            else:
                sums[k] = call(plus_kernel, [like], (halves[k], other), like.size)[0]
                ready.append(sums[k])
    return out


def swap_cores(v, dp):
    return lax.ppermute(v, "dp", [(d, d ^ 1) for d in range(dp)])


def body(
    tokens,
    queries,
    keys,
    values,
    ln_gain,
    mean_in,
    sigma_in,
    noise_in,
    mean_out,
    sigma_out,
    noise_out,
    flip_in,
    flip_mid,
    flip_hidden,
    flip_out,
    cotangent,
):
    own, patches, width = tokens.shape
    rows = own * patches
    seq = lax.axis_size("seq")
    dp = lax.axis_size("dp")
    hidden_local = mean_in.shape[1]
    flat = (rows, width)
    cot_own = cotangent.reshape(flat)

    cot = gather(cot_own, seq, 1)
    pert_in, pert_out = call(
        perturb_kernel,
        [jax.ShapeDtypeStruct(mean_in.shape, BF), jax.ShapeDtypeStruct(mean_out.shape, BF)],
        (sigma_in, noise_in, sigma_out, noise_out),
        4 * sigma_in.size,
    )

    small = jax.ShapeDtypeStruct((rows, hidden_local), BF)
    big = jax.ShapeDtypeStruct(flat, BF)
    resid, normed = call(
        functools.partial(attention_kernel, own),
        [big, big],
        (tokens.reshape(flat), queries.reshape(flat), keys.reshape(flat), values.reshape(flat), ln_gain),
        4 * rows * patches * width,
    )
    act = gather(normed, seq, 2)

    weights = (mean_in, pert_in, mean_out, pert_out)
    flips = (flip_in, flip_mid, flip_hidden, flip_out)
    flop = 8 * rows * width * hidden_local
    hidden, dpre = [], []
    for r in range(seq):
        h, d = call(functools.partial(mlp_kernel, r, own, seq), [small, small], (act[r], cot[r], *weights, *flips), flop)
        hidden.append(h)
        dpre.append(d)

    last = seq - 1
    likes, axes, keeps, sends = [], [], [], []
    for axis, left_sign, right_sign, noise, lefts, rights in (
        (1, flip_hidden, flip_out, noise_out, hidden, cot), (0, flip_in, flip_mid, noise_in, act, dpre)
    ):
        acc = jax.ShapeDtypeStruct(noise.shape, F32)
        early = call(
            functools.partial(early_kernel, tuple(range(last)), own, seq),
            [acc, acc],
            (left_sign, right_sign, *lefts[:last], *rights[:last]),
            last * flop // 2,
        )
        shape = tuple(n // 2 if i == axis else n for i, n in enumerate(noise.shape))
        half = jax.ShapeDtypeStruct(shape, BF)
        for flipped in (0, 1):
            keep, send = call(
                functools.partial(late_kernel, last, own, seq, axis, flipped),
                [half, half],
                (left_sign, right_sign, noise, early[flipped], lefts[last], rights[last]),
                flop // 4,
            )
            likes.append(noise)
            axes.append(axis)
            keeps.append(keep)
            sends.append(send)

    pieces = []
    for keep, send in zip(keeps, sends):
        got = swap_cores(send, dp)
        piece = jax.ShapeDtypeStruct((keep.shape[0] // PIECES, keep.shape[1]), BF)
        pieces += call(split_kernel, [piece] * PIECES, (keep, got), keep.size)
    if dp == 4 * CORES and len({p.shape for p in pieces}) == 1:
        summed = four_line_sums(pieces)
    else:
        summed = [line_sum(p, dp // CORES) for p in pieces]
    swapped = [swap_cores(p, dp) for p in summed]
    grads = []
    for a, (like, axis) in enumerate(zip(likes, axes)):
        full = ()
        for i in range(PIECES):
            c = a * PIECES + i
            full = call(
                assemble_kernel,
                [jax.ShapeDtypeStruct(like.shape, F32)],
                (summed[c], swapped[c], *full),
                like.size,
                grid=(2,),
                in_specs=[VMEM, VMEM] + [pl.BlockSpec(memory_space=pl.ANY)] * len(full),
                out_specs=[pl.BlockSpec(summed[c].shape, functools.partial(block_of, axis, i))],
                input_output_aliases={2: 0} if full else {},
            )
        grads += full

    both = []
    two = jax.ShapeDtypeStruct((2 * rows, width), BF)
    for r in range(seq):
        part = call(functools.partial(partial_kernel, r, own, seq), [two], (hidden[r], dpre[r], *weights, *flips), flop)[0]
        both.append(give(part, r, seq) if r else part)
    block_out, resid_grad = call(
        functools.partial(norm_back_kernel, seq), [big, big], (resid, cot_own, ln_gain, *both), 20 * rows * width
    )
    return (block_out.reshape(tokens.shape), resid_grad.reshape(tokens.shape), grads[2], grads[3], grads[0], grads[1])


def solution(mesh):
    img = P(("dp", "seq"), None, None)
    return jax.shard_map(
        body,
        mesh=mesh,
        in_specs=(
            img,
            img,
            img,
            img,
            P(),
            P(None, "seq"),
            P(None, "seq"),
            P(None, "seq"),
            P("seq", None),
            P("seq", None),
            P("seq", None),
            P("dp", None),
            P("dp", "seq"),
            P("dp", "seq"),
            P("dp", None),
            img,
        ),
        out_specs=(img, img, P(None, "seq"), P(None, "seq"), P("seq", None), P("seq", None)),
        check_vma=False,
    )
```
